32 devices in a mesh: groups: 2 (over x), expert: 8 (over z, y), sub: 2 (over core).
Axes of the slice: x: 2, y: 2, z: 4, core: 2. Of those that a mesh axis runs over, the one named last changes fastest.
Arguments:
- hidden_state: bfloat16 [2048, 2048], P(('groups', 'expert', 'sub')), parts along dimension 0, may hold values from -6 to 6
- norm_gain: float32 [2048], replicated, may hold values from 0.5 to 1.5
- router_weight: bfloat16 [2048, 16], replicated, may hold values from -0.25 to 0.25
- expert_ids: int32 [2048, 6], P(('groups', 'expert', 'sub')), parts along dimension 0, may hold values from 0 to 15, all different within a row; in each aligned block of 64 rows (0 to 63, 64 to 127, ...) at most 32 rows name the same one
- live_counts: int32 [32], P(('groups', 'expert', 'sub')), parts along dimension 0, may hold values from 16 to 64
- routed_gate_up: bfloat16 [16, 2048, 2816], P(('expert', 'sub')), may hold values from -0.125 to 0.125
- routed_down: bfloat16 [16, 1408, 2048], P(('expert', 'sub')), may hold values from -0.15625 to 0.15625
- shared_weights: bfloat16 [3, 2048, 2816], P(None, None, 'expert'), may hold values from -0.125 to 0.125
Outputs:
- mixed: bfloat16 [2048, 2048], P(('groups', 'expert', 'sub')), parts along dimension 0
- penalty: float32 [2], P('groups'), parts along dimension 0
The draws below stay inside these ranges and needn't reach their ends.
There are 2 independent parts, one for each index of `groups`. The reference program is written for one: setup_inputs(seed, part) draws one part's arguments, and reference() takes and returns one part's arrays. A program takes and returns all parts, laid end to end along the dimension named above; an argument that names none is the same for every part. Nothing has to cross between parts.
Inputs may be any that keep to these rules, and one draw needn't show every extreme that they name: `expert_ids`: in each row the 6 experts differ; among the 64 rows of one device no expert is named more than 32 times.
All inputs are finite; a program needn't handle non-finite values.
Results may differ from the reference program's by a relative error of at most 0.0065.
Values may be sent and summed in bfloat16 or wider, within the bound.
A program may use at most 128 MiB of HBM per device.

```python
import math
import jax
import jax.numpy as jnp
import numpy as np
from jax import lax

D = 2048
FF = 1408
SHARED_FF = 2816
TOP = 6
TOK_DEV = 64
EXPERTS = 16
CAP = 32
TOKENS = 1024
N_EXPERT = 8
N_SUB = 2


def draw_live_counts(key, part):
    count = N_EXPERT * N_SUB
    lowest = max(TOK_DEV // 4, 1)
    spread = max(TOK_DEV // 8, 1)
    index = jnp.arange(count, dtype=jnp.int32)
    base = lowest + (TOK_DEV - lowest) * index // (count - 1)
    jitter = jax.random.randint(jax.random.fold_in(key, 17), (count,), -spread, spread + 1, dtype=jnp.int32)
    inner = ((index > 0) & (index < count - 1)).astype(jnp.int32)
    return jnp.clip(base + jitter * inner, lowest, TOK_DEV).astype(jnp.int32)


def level_of(rng, shape, cuts, low, largest):
    gain = 1.0
    for axis_at, blocks in cuts:
        heights = jax.random.uniform(jax.random.fold_in(jax.random.fold_in(rng, 6), axis_at), (blocks,), jnp.float32, low / len(cuts), largest / len(cuts))
        gain = gain * jnp.repeat(jnp.exp(heights), shape[axis_at] // blocks).reshape((-1,) + (1,) * (len(shape) - 1 - axis_at))
    return gain


def deal_out(key, own, number, rows, amount, top, limit, lean):
    order = jax.random.permutation(key, amount)
    crowded, ordinary = portions_of(amount, rows * top, limit, lean, True), portions_of(amount, rows * top, limit, lean, False)
    places = jnp.arange(amount)

    def named(sizes, rotation):
        used = int((sizes > 0).sum())
        fixed = max(1, used // 4)
        moved = fixed + (places - fixed + rotation * (used - fixed)) % max(1, amount - fixed)
        return jnp.zeros((amount,), jnp.int32).at[order[jnp.where(places < fixed, places, moved)]].set(jnp.asarray(sizes, jnp.int32))

    sizes = jnp.where(number % 4 == 0, named(crowded, number // 4), named(ordinary, number - number // 4 - 1))
    mixed = jax.random.permutation(jax.random.fold_in(own, 3), amount)
    donor, receiver = mixed[0:amount // 2 * 2:2], mixed[1:amount // 2 * 2:2]
    margin = jnp.minimum(sizes[donor] - 1, limit - sizes[receiver]) // 2
    margin = jnp.where((donor == order[0]) | (receiver == order[0]) | (sizes[receiver] == 0), 0, jnp.maximum(margin, 0))
    moved = jax.random.randint(jax.random.fold_in(own, 4), (amount // 2,), 0, 1 << 20) % (margin + 1)
    sizes = sizes.at[donor].add(-moved).at[receiver].add(moved)
    items = jnp.searchsorted(jnp.cumsum(sizes), jnp.arange(rows * top), side="right").astype(jnp.int32)
    listing = items.reshape(top, rows).T
    listing = listing[jax.random.permutation(jax.random.fold_in(own, 1), rows)]
    rotation = jax.random.randint(jax.random.fold_in(own, 2), (rows, 1), 0, top)
    return jnp.take_along_axis(listing, (jnp.arange(top)[None, :] + rotation) % top, axis=1)


def portions_of(count, total, bound, lean, full):
    loads = [(1 << 20) // math.isqrt(rank ** lean) + 1 for rank in range(1, count + 1)]
    largest = bound if full else min(bound, max(-(-total // count), total * loads[0] // sum(loads)))
    least = 1 if total - largest >= count - 1 else 0
    counts, rest = [largest] + [least] * (count - 1), total - largest - least * (count - 1)
    while rest > 0:
        candidates = [i for i in range(1, count) if counts[i] < largest] or [i for i in range(1, count) if counts[i] < bound]
        pool, left = sum([loads[i] for i in candidates]), rest
        for i in candidates:
            extra = min(bound - counts[i], max(1, left * loads[i] // pool), rest)
            counts[i] = counts[i] + extra
            rest = rest - extra
    return np.array(counts)


def scatter_about(stream_key, extent, scale, most, cuts=(), kind=jnp.bfloat16):
    level = level_of(stream_key, extent, cuts, -0.22, 0.18) if cuts else 1.0
    entries = jax.random.normal(stream_key, extent, jnp.float32) * scale * level
    return jnp.minimum(jnp.maximum(entries, -most), most).astype(kind)


def setup_inputs(seed: int = 0, part: int = 0) -> dict:
    keys = jax.random.split(jax.random.key(seed), 9)
    own_keys = jax.random.split(jax.random.fold_in(keys[8], part), 9)
    hidden_state = scatter_about(own_keys[0], (TOKENS, D), 1.0, 6.0, ((0, 16),))
    norm_gain = jnp.clip(1.0 + 0.1 * jax.random.normal(keys[1], (D,), jnp.float32), 0.5, 1.5)
    router_weight = scatter_about(keys[2], (D, EXPERTS), (D // 4) ** -0.5, 0.25)
    expert_ids_keys = jax.random.split(jax.random.fold_in(own_keys[3], 1), TOKENS // TOK_DEV)
    expert_ids_turns = jax.random.permutation(jax.random.fold_in(own_keys[3], 3), TOKENS // TOK_DEV)
    expert_ids = jax.vmap(lambda own, number: deal_out(jax.random.fold_in(own_keys[3], 2), own, number, TOK_DEV, EXPERTS, TOP, CAP, 1))(expert_ids_keys, expert_ids_turns).reshape((TOKENS, TOP))
    live_counts = draw_live_counts(jax.random.fold_in(jax.random.fold_in(keys[8], part), 71), part)
    routed_gate_up = scatter_about(keys[5], (EXPERTS, D, 2 * FF), D ** -0.5, 0.125, ((0, 16),))
    routed_down = scatter_about(keys[6], (EXPERTS, FF, D), FF ** -0.5, 0.15625, ((0, 16),))
    shared_weights = scatter_about(keys[7], (3, D, SHARED_FF), D ** -0.5, 0.125, ((2, 8),))
    return {"hidden_state": hidden_state, "norm_gain": norm_gain, "router_weight": router_weight, "expert_ids": expert_ids, "live_counts": live_counts, "routed_gate_up": routed_gate_up, "routed_down": routed_down, "shared_weights": shared_weights}


def normalize(states, norm_gain):
    values = states.astype(jnp.float32)
    spread = lax.optimization_barrier(jnp.mean(values * values, axis=-1, keepdims=True))
    return (values * lax.rsqrt(spread + 1e-06) * norm_gain).astype(jnp.bfloat16)

def expert_ffn(packed):
    inputs, gate_up, down_proj = packed
    inner = jnp.dot(inputs, gate_up, preferred_element_type=jnp.float32)
    active = (jax.nn.silu(inner[:, :FF]) * inner[:, FF:]).astype(jnp.bfloat16)
    return jnp.dot(active, down_proj, preferred_element_type=jnp.float32).astype(jnp.bfloat16)

def reference(hidden_state, norm_gain, router_weight, expert_ids, live_counts, routed_gate_up, routed_down, shared_weights):
    devices = N_EXPERT * N_SUB
    normed = normalize(hidden_state, norm_gain)
    probs = jax.nn.sigmoid(jnp.dot(normed, router_weight, preferred_element_type=jnp.float32))
    positions = jnp.arange(TOKENS, dtype=jnp.int32)
    owners = positions // TOK_DEV
    live = (positions % TOK_DEV < live_counts[owners]).astype(jnp.float32)
    columns = jnp.arange(EXPERTS, dtype=jnp.int32)
    onehot = (expert_ids[:, :, None] == columns[None, None, :]).astype(jnp.int32)
    picked = lax.optimization_barrier(jnp.sum(onehot.astype(jnp.float32) * probs[:, None, :], axis=-1))
    weights = (live[:, None] * picked / lax.optimization_barrier(jnp.sum(picked, axis=-1, keepdims=True))).astype(jnp.bfloat16)
    live_hot = onehot * live.astype(jnp.int32)[:, None, None]
    per_device = live_hot.reshape(devices, TOK_DEV * TOP, EXPERTS)
    ranks = jnp.cumsum(per_device, axis=1) - per_device
    slot = lax.optimization_barrier(jnp.sum(ranks * per_device, axis=-1)).reshape(devices, TOK_DEV, TOP)
    places = expert_ids.reshape(devices, TOK_DEV, TOP) * CAP + slot
    valid = live.reshape(devices, TOK_DEV, 1, 1)
    cells = jnp.arange(EXPERTS * CAP, dtype=jnp.int32)
    match = (places[..., None] == cells[None, None, None, :]).astype(jnp.float32)
    table = lax.optimization_barrier(jnp.sum(match, axis=2)) * valid[:, :, 0]
    buffer = jnp.einsum('dtc,dtf->dcf', table, normed.reshape(devices, TOK_DEV, D).astype(jnp.float32)).astype(jnp.bfloat16)
    buffer = buffer.reshape(devices, EXPERTS, CAP, D).transpose(1, 0, 2, 3).reshape(EXPERTS, devices * CAP, D)
    outputs = lax.map(expert_ffn, (buffer, routed_gate_up, routed_down))
    outputs = outputs.reshape(EXPERTS, devices, CAP, D).transpose(1, 0, 2, 3).reshape(devices, EXPERTS * CAP, D)
    mixing = lax.optimization_barrier(jnp.sum(match * weights.reshape(devices, TOK_DEV, TOP, 1).astype(jnp.float32), axis=2))
    routed = jnp.einsum('dtc,dcf->dtf', mixing, outputs.astype(jnp.float32)).reshape(TOKENS, D)
    gate_part = jnp.dot(normed, shared_weights[0], preferred_element_type=jnp.float32)
    up_part = jnp.dot(normed, shared_weights[1], preferred_element_type=jnp.float32)
    shared_active = (jax.nn.silu(gate_part) * up_part).astype(jnp.bfloat16)
    shared_out = lax.dot_general(shared_active, shared_weights[2], (((1,), (1,)), ((), ())), preferred_element_type=jnp.float32)
    mixed = (shared_out + routed).astype(jnp.bfloat16)
    load = lax.optimization_barrier(jnp.sum(live_hot.astype(jnp.float32), axis=(0, 1)))
    mass = lax.optimization_barrier(jnp.sum(probs * live[:, None], axis=0))
    penalty = EXPERTS * jnp.sum(load * mass) / (TOP * float(TOKENS) * float(TOKENS))
    return (mixed, penalty.reshape(1))
```

```python
import functools

import jax
import jax.numpy as jnp
from jax import lax
from jax.experimental import pallas as pl
from jax.experimental.pallas import tpu as pltpu
from jax.sharding import PartitionSpec as P

MESH = pl.DeviceIdType.MESH
LANES = 128
SLOTS = 5


def ring_place(chip, chips, fold):
    if fold == 1:
        return chip
    row, step = chip % 2, chip // 2
    return (1 - row) * step + row * (chips - 1 - step)


def ring_chip(place, chips, fold):
    if fold == 1:
        return place
    back = place // (chips // 2)
    step = (1 - back) * place + back * (chips - 1 - place)
    return 2 * step + back


class Plan:
    def __init__(self, chips, fold, tok, width, units, shared, choose, experts):
        self.chips, self.fold, self.hops = chips, fold, chips // 2
        self.tok, self.width, self.half = tok, width, tok // 2
        self.units, self.shared, self.choose, self.experts = units, shared, choose, experts
        self.sublanes = -(-experts // 16) * 16
        hops = self.hops
        order = [(0, 0), (0, 1)]
        for hop, j in (
            [(1, 0), (1, 1)]
            + [(h, 0) for h in range(2, hops + 1)]
            + [(h, 1) for h in range(2, hops + 1)]
        ):
            order.append((hop, j))
            if hop < hops:
                order.append((chips - hop, j))
        self.order = order
        self.group = 4
        self.steps = len(order) // self.group
        self.rows = self.group * 2 * self.half
        self.routed_tiles = units // LANES
        full = shared // LANES
        self.pairs = full // 2
        self.rest = [
            (at, min(LANES, shared - at)) for at in range(self.pairs * 2 * LANES, shared, LANES)
        ]
        self.tiles = self.routed_tiles + self.pairs + len(self.rest)
        self.depth = self.tiles * LANES
        self.downs = width // 256

    def index(self, k, j):
        return self.order.index((k % self.chips, j))

    def span(self, r, k, j):
        return pl.ds((2 * self.index(k, j) + r) * self.half, self.half)

    def cols(self, c):
        return pl.ds(c * (self.width // 2), self.width // 2)

    def step_of(self, k, j):
        return self.index(k, j) // self.group


def silu(v):
    return v / (1.0 + jnp.exp(-v))


def layer_kernel(
    plan, hid_hbm, gain_hbm, router_hbm, ids_hbm, live_ref, gu_hbm, dn_hbm, sh_hbm,
    out_ref, pen_ref,
    hid, gain, router, ids, square, notes, wt, wd, stage, x_all, y_all, from_peer, going, coming,
    act, rbuf, scale, in_sem, w_sem, gs, gr, ps, pr, ys, yr, ss, sr,
):
    chips, fold, hops, half = plan.chips, plan.fold, plan.hops, plan.half
    tok, width, tiles = plan.tok, plan.width, plan.tiles
    sub = lax.axis_index("sub")
    chip = lax.axis_index("expert")
    me = chip * 2 + sub
    place = ring_place(chip, chips, fold)
    right = ring_chip((place + 1) % chips, chips, fold)
    left = ring_chip((place + chips - 1) % chips, chips, fold)
    along = [{"expert": right, "sub": sub}, {"expert": left, "sub": sub}]
    peer = {"expert": chip, "sub": 1 - sub}
    sign = (-1, 1)

    def remote(src, dst, send, recv, device):
        return pltpu.make_async_remote_copy(
            src_ref=src, dst_ref=dst, send_sem=send, recv_sem=recv,
            device_id=device, device_id_type=MESH,
        )

    def gather_copy(way, hop, j):
        cols = plan.cols(way) if hop == hops else pl.ds(0, width)
        src = x_all.at[plan.span(0, sign[way] * (hop - 1), j), cols]
        dst = x_all.at[plan.span(0, sign[way] * hop, j), cols]
        return remote(src, dst, gs.at[way, hop - 1, j], gr.at[way, hop - 1, j], along[way])

    def note_copy(way, hop):
        src = notes.at[0, sign[way] * (hop - 1) % chips]
        dst = notes.at[0, sign[way] * hop % chips]
        return remote(src, dst, gs.at[way, hop - 1, 2], gr.at[way, hop - 1, 2], along[way])

    def peer_copies(k, j):
        k = k % chips
        parts = (0, 1) if k == hops else (2,)
        made = []
        for c in parts:
            cols = pl.ds(0, width) if c == 2 else plan.cols(c)
            at = 2 * j + c % 2
            made.append(
                remote(
                    x_all.at[plan.span(0, k, j), cols], x_all.at[plan.span(1, k, j), cols],
                    ps.at[k, at], pr.at[k, at], peer,
                )
            )
        return made

    def peer_note(k):
        k = k % chips
        return remote(notes.at[0, k], notes.at[1, k], ps.at[k, 4], pr.at[k, 4], peer)

    def part_copy(q, c):
        cols = plan.cols(c)
        if isinstance(q, int):
            src, dst = pl.ds((2 * q + 1) * half, half), pl.ds(q * half, half)
        else:
            src = pl.ds(pl.multiple_of((2 * q + 1) * half, half), half)
            dst = pl.ds(pl.multiple_of(q * half, half), half)
        return remote(
            y_all.at[src, cols], from_peer.at[dst, cols], ys.at[q, c], yr.at[q, c], peer
        )

    def sum_copy(way, hop, j, c):
        spot = (way, hop - 1, pl.ds(j * half, half), plan.cols(c))
        at = 2 * j + c
        return remote(
            going.at[spot], coming.at[spot], ss.at[way, hop - 1, at], sr.at[way, hop - 1, at],
            along[way],
        )

    def ways_of(hop, c):
        return (c,) if hop == hops else (0, 1)

    small = [
        pltpu.make_async_copy(hid_hbm, hid, in_sem.at[0]),
        pltpu.make_async_copy(gain_hbm, gain, in_sem.at[1]),
        pltpu.make_async_copy(router_hbm, router, in_sem.at[2]),
        pltpu.make_async_copy(ids_hbm, ids, in_sem.at[3]),
        pltpu.make_async_copy(sh_hbm, stage, in_sem.at[4]),
    ]
    down_load = pltpu.make_async_copy(dn_hbm.at[0], wd.at[pl.ds(0, plan.units)], in_sem.at[5])

    def tile_loads(n):
        if n < plan.routed_tiles:
            return [
                pltpu.make_async_copy(
                    gu_hbm.at[0, :, pl.ds(side * plan.units + n * LANES, LANES)],
                    wt.at[n, :, pl.ds(side * LANES, LANES)], w_sem.at[n, side],
                )
                for side in range(2)
            ]
        return []

    for copy in small[:4]:
        copy.start()
    barrier = pltpu.get_barrier_semaphore()
    for target in along + [peer]:
        pl.semaphore_signal(barrier, inc=1, device_id=target, device_id_type=MESH)
    small[4].start()
    for n in range(tiles):
        for copy in tile_loads(n):
            copy.start()
    down_load.start()

    small[0].wait()
    small[1].wait()
    for j in range(2):
        values = hid[pl.ds(j * half, half), :].astype(jnp.float32)
        spread = jnp.mean(values * values, axis=-1, keepdims=True)
        x_all[plan.span(0, 0, j), :] = (
            values * lax.rsqrt(spread + 1e-06) * gain[...]
        ).astype(jnp.bfloat16)
    pl.semaphore_wait(barrier, 3)
    for way in range(2):
        if hops > 1 or way == 0:
            gather_copy(way, 1, 0).start()
    for copy in peer_copies(0, 0):
        copy.start()

    small[2].wait()
    small[3].wait()
    experts = plan.experts
    columns = lax.broadcasted_iota(jnp.int32, (half, experts), 1)
    square[...] = jnp.zeros_like(square)
    load = jnp.zeros((1, experts), jnp.float32)
    mass = jnp.zeros((1, experts), jnp.float32)
    for j in range(2):
        normed = x_all[plan.span(0, 0, j), :]
        logits = jnp.dot(normed, router[...], preferred_element_type=jnp.float32)
        probs = 1.0 / (1.0 + jnp.exp(-logits))
        named = ids[pl.ds(j * half, half), :]
        hot = jnp.zeros((half, experts), jnp.float32)
        for k in range(plan.choose):
            hot = hot + jnp.where(named[:, k : k + 1] == columns, 1.0, 0.0)
        token = lax.broadcasted_iota(jnp.int32, (half, experts), 0) + j * half
        live = jnp.where(token < live_ref[0], 1.0, 0.0)
        picked = hot * probs
        weights = live * picked / jnp.sum(picked, axis=-1, keepdims=True)
        square[pl.ds(j * half, half), pl.ds(0, experts)] = weights
        load = load + jnp.sum(hot * live, axis=0, keepdims=True)
        mass = mass + jnp.sum(probs * live, axis=0, keepdims=True)
    square[pl.ds(tok, 1), pl.ds(0, experts)] = load
    for at in range(3):
        kept = mass.astype(jnp.bfloat16).astype(jnp.float32)
        square[pl.ds(tok + 1 + at, 1), pl.ds(0, experts)] = kept
        mass = mass - kept
    turned = jnp.transpose(square[...])
    notes[0, 0] = turned[: plan.sublanes].astype(jnp.bfloat16)
    for way in range(2):
        if hops > 1 or way == 0:
            note_copy(way, 1).start()
        if hops > 1 or way == 1:
            gather_copy(way, 1, 1).start()
    peer_note(0).start()
    for copy in peer_copies(0, 1):
        copy.start()

    small[4].wait()
    for i in range(plan.pairs):
        lanes = pl.ds(pl.multiple_of((2 * i + sub) * LANES, LANES), LANES)
        n = plan.routed_tiles + i
        for side in range(2):
            wt[n, :, pl.ds(side * LANES, LANES)] = stage[side, :, lanes]
        wd[pl.ds(n * LANES, LANES), :] = jnp.transpose(stage[2, :, lanes])
    for i, (at, wide) in enumerate(plan.rest):
        n = plan.routed_tiles + plan.pairs + i
        if wide < LANES:
            wt[n] = jnp.zeros_like(wt[n])
        for side in range(2):
            wt[n, :, pl.ds(side * LANES, wide)] = stage[side, :, pl.ds(at, wide)]
        wd[pl.ds(n * LANES, wide), :] = jnp.transpose(stage[2, :, pl.ds(at, wide)])
        if wide < LANES:
            wd[pl.ds(n * LANES + wide, LANES - wide), :] = jnp.zeros(
                (LANES - wide, width), jnp.bfloat16
            )

    events = {}

    def at_slot(spot, event):
        events.setdefault(spot, []).append(event)

    def arrive(hop, j):
        for way in range(2):
            k = sign[way] * hop
            if j == 0 and (hop < hops or way == 0):
                note_copy(way, hop).wait_recv()
                if hop + 1 < hops or (hop + 1 == hops and way == 0):
                    note_copy(way, hop + 1).start()
                peer_note(k).start()
            gather_copy(way, hop, j).wait_recv()
            if hop + 1 <= hops:
                gather_copy(way, hop + 1, j).start()
            made = peer_copies(k, j)
            (made[way] if hop == hops else made[0]).start()

    def ready(step):
        for i in range(plan.group):
            k, j = plan.order[step * plan.group + i]
            for copy in peer_copies(k, j):
                copy.wait_recv()
            if j == 0:
                peer_note(k).wait_recv()
            for r in range(2):
                tile = notes[r, k].astype(jnp.float32)
                mine = lax.broadcasted_iota(jnp.int32, tile.shape, 0) == me
                line = jnp.sum(jnp.where(mine, tile, 0.0), axis=0, keepdims=True)
                row = lax.broadcasted_iota(jnp.int32, (half, LANES), 0) + j * half
                lane = lax.broadcasted_iota(jnp.int32, (half, LANES), 1)
                column = jnp.sum(jnp.where(row == lane, line, 0.0), axis=1, keepdims=True)
                scale[pl.ds((2 * i + r) * half, half), :] = jnp.broadcast_to(column, (half, LANES))

    arrivals = [(h, j) for h in range(1, hops + 1) for j in range(2)]
    wanted = [0, 1, 3, 6, 8, 10, 10, 11]
    spots = []
    for i, (hop, j) in enumerate(arrivals):
        due = SLOTS * min(plan.step_of(hop, j), plan.step_of(-hop, j))
        spots.append(min(due, wanted[i] if i < len(wanted) else 2 * i))
    for i in reversed(range(len(spots) - 1)):
        spots[i] = min(spots[i], spots[i + 1])
    for (hop, j), spot in zip(arrivals, spots):
        at_slot(spot, functools.partial(arrive, hop, j))
    for step in range(plan.steps):
        at_slot(SLOTS * step, functools.partial(ready, step))
    quarter = 4

    def loads(first, last):
        for n in range(first, min(last, tiles)):
            for copy in tile_loads(n):
                copy.wait()

    for part in range(3):
        last = tiles if part == 2 else quarter * (part + 1)
        at_slot(part, functools.partial(loads, quarter * part, last))
    at_slot(2, down_load.wait)

    def own_part(k, j, c):
        q = plan.index(k, j)
        part_copy(q, c).wait_recv()
        value = y_all[plan.span(0, k, j), plan.cols(c)].astype(jnp.float32)
        return value + from_peer[pl.ds(q * half, half), plan.cols(c)].astype(jnp.float32)

    def pass_on(hop, j):
        for c in range(2):
            shared = None
            for way in ways_of(hop, c):
                k = -sign[way] * hop
                value = own_part(k, j, c)
                if hop < hops and way in ways_of(hop + 1, c):
                    sum_copy(way, hop + 1, j, c).wait_recv()
                    spot = (way, hop, pl.ds(j * half, half), plan.cols(c))
                    value = value + coming[spot].astype(jnp.float32)
                spot = (way, hop - 1, pl.ds(j * half, half), plan.cols(c))
                going[spot] = value.astype(going.dtype)
                sum_copy(way, hop, j, c).start()

    def finish(j):
        for c in range(2):
            value = own_part(0, j, c)
            for way in ways_of(1, c):
                sum_copy(way, 1, j, c).wait_recv()
                spot = (way, 0, pl.ds(j * half, half), plan.cols(c))
                value = value + coming[spot].astype(jnp.float32)
            out_ref[pl.ds(j * half, half), plan.cols(c)] = value.astype(out_ref.dtype)

    first = [functools.partial(pass_on, h, 0) for h in range(hops, 0, -1)]
    first.append(functools.partial(finish, 0))
    second = [functools.partial(pass_on, h, 1) for h in range(hops, 0, -1)]
    second.append(functools.partial(finish, 1))
    spot = SLOTS * (plan.step_of(hops, 0) + 1) + 1
    while EARLY and spot < SLOTS * plan.steps and len(first) > 1:
        at_slot(spot, first.pop(0))
        spot += 3

    def run(t, slot):
        for step in range(plan.steps):
            todo = events.get(SLOTS * step + slot, [])
            if todo:

                @pl.when(t == step)
                def _():
                    for event in todo:
                        event()

    own_row = (lax.broadcasted_iota(jnp.int32, (plan.rows, LANES), 0) // half) % 2 == 0
    lane = lax.broadcasted_iota(jnp.int32, (plan.rows, LANES), 1)

    def activate(n):
        both = rbuf[...]
        value = silu(both[:, :LANES]) * both[:, LANES:]
        if n < plan.routed_tiles:
            value = value * scale[...]
        elif n >= plan.routed_tiles + plan.pairs:
            wide = plan.rest[n - plan.routed_tiles - plan.pairs][1]
            value = jnp.where(own_row & (lane < wide), value, 0.0)
        act[:, pl.ds(n * LANES, LANES)] = value.astype(jnp.bfloat16)

    def step_body(t, carry):
        rows = pl.ds(pl.multiple_of(t * plan.rows, plan.rows), plan.rows)
        run(t, 0)
        for n in range(tiles):
            if n > 0:
                activate(n - 1)
            rbuf[...] = jnp.dot(x_all[rows, :], wt[n], preferred_element_type=jnp.float32)
            if (n + 1) % quarter == 0 and (n + 1) // quarter < SLOTS - 1:
                run(t, (n + 1) // quarter)
        activate(tiles - 1)
        for n in range(plan.downs):
            cols = pl.ds(n * 256, 256)
            y_all[rows, cols] = jnp.dot(
                act[...], wd[:, cols], preferred_element_type=jnp.float32
            ).astype(jnp.bfloat16)
            if 2 * (n + 1) == plan.downs:
                for i in range(plan.group):
                    part_copy(plan.group * t + i, 0).start()
                run(t, SLOTS - 1)
        for i in range(plan.group):
            part_copy(plan.group * t + i, 1).start()
        return carry

    lax.fori_loop(0, plan.steps, step_body, 0)

    while first or second:
        if second and len(second) >= len(first):
            second.pop(0)()
        else:
            first.pop(0)()

    total = jnp.zeros((plan.sublanes, LANES), jnp.float32)
    for r in range(2):
        for k in range(chips):
            total = total + notes[r, k].astype(jnp.float32)
    mass = total[:, tok + 1 : tok + 2] + total[:, tok + 2 : tok + 3] + total[:, tok + 3 : tok + 4]
    every = float(tok * chips * 2)
    penalty = experts * jnp.sum(total[:, tok : tok + 1] * mass) / (plan.choose * every * every)
    pen_ref[0] = penalty

    for hop in range(1, hops + 1):
        for way in range(2):
            for j in range(2):
                gather_copy(way, hop, j).wait_send()
            if hop < hops or way == 0:
                note_copy(way, hop).wait_send()
            for j in range(2):
                for c in range(2):
                    if way in ways_of(hop, c):
                        sum_copy(way, hop, j, c).wait_send()
    for k in range(chips):
        peer_note(k).wait_send()
        for j in range(2):
            for copy in peer_copies(k, j):
                copy.wait_send()
    for q in range(len(plan.order)):
        for c in range(2):
            part_copy(q, c).wait_send()


EARLY = True


def on_device(
    fold, hidden_state, norm_gain, router_weight, expert_ids, live_counts,
    routed_gate_up, routed_down, shared_weights,
):
    tok, width = hidden_state.shape
    chips, subs = lax.axis_size("expert"), lax.axis_size("sub")
    units, shared = routed_down.shape[1], shared_weights.shape[2]
    if subs != 2 or chips % 4 or routed_gate_up.shape[0] != 1 or tok + 4 > LANES:
        raise ValueError("unsupported sizes")
    plan = Plan(
        chips, fold, tok, width, units, shared, expert_ids.shape[1], router_weight.shape[1]
    )
    hops, count = plan.hops, len(plan.order)
    bf16, f32 = jnp.bfloat16, jnp.float32
    hbm = pl.BlockSpec(memory_space=pl.ANY)
    dma = pltpu.SemaphoreType.DMA
    mixed, penalty = pl.pallas_call(
        functools.partial(layer_kernel, plan),
        out_shape=(
            jax.ShapeDtypeStruct((tok, width), bf16),
            jax.ShapeDtypeStruct((1,), f32),
        ),
        in_specs=[hbm] * 4 + [pl.BlockSpec(memory_space=pltpu.SMEM)] + [hbm] * 3,
        out_specs=(
            pl.BlockSpec(memory_space=pltpu.VMEM),
            pl.BlockSpec(memory_space=pltpu.SMEM),
        ),
        scratch_shapes=[
            pltpu.VMEM((tok, width), bf16),
            pltpu.VMEM((1, width), f32),
            pltpu.VMEM(router_weight.shape, bf16),
            pltpu.VMEM(expert_ids.shape, jnp.int32),
            pltpu.VMEM((LANES, LANES), f32),
            pltpu.VMEM((2, chips, plan.sublanes, LANES), bf16),
            pltpu.VMEM((plan.tiles, width, 2 * LANES), bf16),
            pltpu.VMEM((plan.depth, width), bf16),
            pltpu.VMEM(shared_weights.shape, bf16),
            pltpu.VMEM((count * 2 * plan.half, width), bf16),
            pltpu.VMEM((count * 2 * plan.half, width), bf16),
            pltpu.VMEM((count * plan.half, width), bf16),
            pltpu.VMEM((2, hops, tok, width), bf16),
            pltpu.VMEM((2, hops, tok, width), bf16),
            pltpu.VMEM((plan.rows, plan.depth), bf16),
            pltpu.VMEM((plan.rows, 2 * LANES), f32),
            pltpu.VMEM((plan.rows, LANES), f32),
            dma((6,)),
            dma((plan.tiles, 2)),
            dma((2, hops, 3)),
            dma((2, hops, 3)),
            dma((chips, 5)),
            dma((chips, 5)),
            dma((count, 2)),
            dma((count, 2)),
            dma((2, hops, 4)),
            dma((2, hops, 4)),
        ],
        compiler_params=pltpu.CompilerParams(
            collective_id=0, has_side_effects=True, vmem_limit_bytes=64 * 1024 * 1024 - 65536
        ),
        name="moe_layer",
    )(
        hidden_state, norm_gain.reshape(1, width), router_weight, expert_ids, live_counts,
        routed_gate_up, routed_down, shared_weights,
    )
    return mixed, penalty


def fold_of(mesh):
    chips = mesh.shape["expert"]
    try:
        spots = [tuple(d.coords) for d in mesh.devices[0, :, 0].flat]
    except (AttributeError, TypeError, ValueError):
        spots = []
    if chips % 2 or chips < 4:
        return 1
    if len(spots) == chips:
        apart = sum(abs(a - b) for a, b in zip(spots[0], spots[2]))
        return 2 if apart == 1 else 1
    return 1


def solution(mesh):
    placed = (
        P(("groups", "expert", "sub"), None),
        P(),
        P(),
        P(("groups", "expert", "sub"), None),
        P(("groups", "expert", "sub")),
        P(("expert", "sub"), None, None),
        P(("expert", "sub"), None, None),
        P(None, None, "expert"),
    )
    return jax.shard_map(
        functools.partial(on_device, fold_of(mesh)),
        mesh=mesh,
        in_specs=placed,
        out_specs=(P(("groups", "expert", "sub"), None), P("groups")),
        check_vma=False,
    )
```

```python
import functools

import jax
import jax.numpy as jnp
from jax import lax
from jax.experimental import pallas as pl
from jax.experimental.pallas import tpu as pltpu
from jax.sharding import PartitionSpec as P

MESH = pl.DeviceIdType.MESH
LANES = 128
SLOTS = 5
GATHER = (1, 2, 2, 4, 4, 5, 6, 7, 8, 9, 10, 11)
SCATTER = (1, 1, 4, 4)


def ring_place(chip, chips, fold):
    if fold == 1:
        return chip
    row, step = chip % 2, chip // 2
    return (1 - row) * step + row * (chips - 1 - step)


def ring_chip(place, chips, fold):
    if fold == 1:
        return place
    back = place // (chips // 2)
    step = (1 - back) * place + back * (chips - 1 - place)
    return 2 * step + back


class Plan:
    def __init__(self, chips, fold, tok, width, units, shared, choose, experts):
        self.chips, self.fold, self.hops = chips, fold, chips // 2
        self.tok, self.width, self.half = tok, width, tok // 2
        self.units, self.shared, self.choose, self.experts = units, shared, choose, experts
        self.sublanes = -(-experts // 16) * 16
        hops = self.hops
        order = [(0, 0), (0, 1)]
        for hop, j in (
            [(1, 0), (1, 1)]
            + [(h, 0) for h in range(2, hops + 1)]
            + [(h, 1) for h in range(2, hops + 1)]
        ):
            order.append((hop, j))
            if hop < hops:
                order.append((chips - hop, j))
        self.order = order
        self.group = 4
        self.steps = len(order) // self.group
        self.rows = self.group * 2 * self.half
        self.routed_tiles = units // LANES
        full = shared // LANES
        self.pairs = full // 2
        self.rest = [
            (at, min(LANES, shared - at)) for at in range(self.pairs * 2 * LANES, shared, LANES)
        ]
        self.tiles = self.routed_tiles + self.pairs + len(self.rest)
        self.depth = self.tiles * LANES
        self.downs = width // 256

    def index(self, k, j):
        return self.order.index((k % self.chips, j))

    def span(self, r, k, j):
        return pl.ds((2 * self.index(k, j) + r) * self.half, self.half)

    def cols(self, c):
        return pl.ds(c * (self.width // 2), self.width // 2)

    def step_of(self, k, j):
        return self.index(k, j) // self.group


def silu(v):
    return v / (1.0 + jnp.exp(-v))


def layer_kernel(
    plan, hid_hbm, gain_hbm, router_hbm, ids_hbm, live_ref, gu_hbm, dn_hbm, sh_hbm,
    out_ref, pen_ref,
    hid, gain, router, ids, square, notes, wt, wd, stage, x_all, y_all, from_peer, going, coming,
    act, rbuf, scale, in_sem, w_sem, gs, gr, ps, pr, ys, yr, ss, sr,
):
    chips, fold, hops, half = plan.chips, plan.fold, plan.hops, plan.half
    tok, width, tiles = plan.tok, plan.width, plan.tiles
    sub = lax.axis_index("sub")
    chip = lax.axis_index("expert")
    me = chip * 2 + sub
    place = ring_place(chip, chips, fold)
    right = ring_chip((place + 1) % chips, chips, fold)
    left = ring_chip((place + chips - 1) % chips, chips, fold)
    along = [{"expert": right, "sub": sub}, {"expert": left, "sub": sub}]
    peer = {"expert": chip, "sub": 1 - sub}
    sign = (-1, 1)

    def remote(src, dst, send, recv, device):
        return pltpu.make_async_remote_copy(
            src_ref=src, dst_ref=dst, send_sem=send, recv_sem=recv,
            device_id=device, device_id_type=MESH,
        )

    def gather_copy(way, hop, j, c):
        cols, at = plan.cols(c), 2 * j + c
        src = x_all.at[plan.span(0, sign[way] * (hop - 1), j), cols]
        dst = x_all.at[plan.span(0, sign[way] * hop, j), cols]
        return remote(src, dst, gs.at[way, hop - 1, at], gr.at[way, hop - 1, at], along[way])

    def note_copy(way, hop):
        src = notes.at[0, sign[way] * (hop - 1) % chips]
        dst = notes.at[0, sign[way] * hop % chips]
        return remote(src, dst, gs.at[way, hop - 1, 4], gr.at[way, hop - 1, 4], along[way])

    def peer_copy(k, j, c):
        k, cols, at = k % chips, plan.cols(c), 2 * j + c
        return remote(
            x_all.at[plan.span(0, k, j), cols], x_all.at[plan.span(1, k, j), cols],
            ps.at[k, at], pr.at[k, at], peer,
        )

    def peer_note(k):
        k = k % chips
        return remote(notes.at[0, k], notes.at[1, k], ps.at[k, 4], pr.at[k, 4], peer)

    def part_copy(q, c):
        cols = plan.cols(c)
        if isinstance(q, int):
            src, dst = pl.ds((2 * q + 1) * half, half), pl.ds(q * half, half)
        else:
            src = pl.ds(pl.multiple_of((2 * q + 1) * half, half), half)
            dst = pl.ds(pl.multiple_of(q * half, half), half)
        return remote(
            y_all.at[src, cols], from_peer.at[dst, cols], ys.at[q, c], yr.at[q, c], peer
        )

    def sum_copy(way, hop, j, c):
        spot = (way, hop - 1, pl.ds(j * half, half), plan.cols(c))
        at = 2 * j + c
        return remote(
            going.at[spot], coming.at[spot], ss.at[way, hop - 1, at], sr.at[way, hop - 1, at],
            along[way],
        )

    def side_of(way, part):
        return way if part == 0 else 1 - way

    def ways_of(hop, c):
        return (c,) if hop == hops else (0, 1)

    small = [
        pltpu.make_async_copy(hid_hbm, hid, in_sem.at[0]),
        pltpu.make_async_copy(gain_hbm, gain, in_sem.at[1]),
        pltpu.make_async_copy(router_hbm, router, in_sem.at[2]),
        pltpu.make_async_copy(ids_hbm, ids, in_sem.at[3]),
        pltpu.make_async_copy(sh_hbm.at[0], stage.at[0], in_sem.at[4]),
        pltpu.make_async_copy(sh_hbm.at[1], stage.at[1], in_sem.at[5]),
    ]
    down_loads = [pltpu.make_async_copy(dn_hbm.at[0], wd.at[pl.ds(0, plan.units)], in_sem.at[6])]
    for i in range(plan.pairs):
        down_loads.append(
            pltpu.make_async_copy(
                sh_hbm.at[2, pl.ds(pl.multiple_of((2 * i + sub) * LANES, LANES), LANES)],
                wd.at[pl.ds(plan.units + i * LANES, LANES)], in_sem.at[7 + i],
            )
        )
    for i, (at, wide) in enumerate(plan.rest):
        n = plan.routed_tiles + plan.pairs + i
        down_loads.append(
            pltpu.make_async_copy(
                sh_hbm.at[2, pl.ds(at, wide)], wd.at[pl.ds(n * LANES, wide)],
                in_sem.at[7 + plan.pairs + i],
            )
        )

    def tile_loads(n):
        if n < plan.routed_tiles:
            return [
                pltpu.make_async_copy(
                    gu_hbm.at[0, :, pl.ds(side * plan.units + n * LANES, LANES)],
                    wt.at[n, :, pl.ds(side * LANES, LANES)], w_sem.at[n, side],
                )
                for side in range(2)
            ]
        return []

    for copy in small[:4]:
        copy.start()
    barrier = pltpu.get_barrier_semaphore()
    for target in along + [peer]:
        pl.semaphore_signal(barrier, inc=1, device_id=target, device_id_type=MESH)
    small[4].start()
    small[5].start()
    for n in range(tiles):
        for copy in tile_loads(n):
            copy.start()
    for copy in down_loads:
        copy.start()

    small[0].wait()
    small[1].wait()
    for j in range(2):
        values = hid[pl.ds(j * half, half), :].astype(jnp.float32)
        spread = jnp.mean(values * values, axis=-1, keepdims=True)
        x_all[plan.span(0, 0, j), :] = (
            values * lax.rsqrt(spread + 1e-06) * gain[...]
        ).astype(jnp.bfloat16)
    pl.semaphore_wait(barrier, 3)
    for part in range(2):
        for way in range(2):
            gather_copy(way, 1, 0, side_of(way, part)).start()
    for c in range(2):
        peer_copy(0, 0, c).start()

    small[2].wait()
    small[3].wait()
    experts = plan.experts
    expert = lax.broadcasted_iota(jnp.int32, (experts, half), 0)
    square[...] = jnp.zeros_like(square)
    load = jnp.zeros((experts, 1), jnp.float32)
    mass = jnp.zeros((experts, 1), jnp.float32)
    named = ids[...]
    for j in range(2):
        logits = lax.dot_general(
            router[...], x_all[plan.span(0, 0, j), :], (((1,), (1,)), ((), ())),
            preferred_element_type=jnp.float32,
        )
        probs = 1.0 / (1.0 + jnp.exp(-logits))
        hot = jnp.zeros((experts, half), jnp.float32)
        for k in range(plan.choose):
            hot = hot + jnp.where(named[k : k + 1, j * half : (j + 1) * half] == expert, 1.0, 0.0)
        token = lax.broadcasted_iota(jnp.int32, (experts, half), 1) + j * half
        live = jnp.where(token < live_ref[0], 1.0, 0.0)
        picked = hot * probs
        weights = live * picked / jnp.sum(picked, axis=0, keepdims=True)
        square[pl.ds(0, experts), pl.ds(j * half, half)] = weights
        load = load + jnp.sum(hot * live, axis=1, keepdims=True)
        mass = mass + jnp.sum(probs * live, axis=1, keepdims=True)
    square[pl.ds(0, experts), pl.ds(tok, 1)] = load
    for at in range(3):
        kept = mass.astype(jnp.bfloat16).astype(jnp.float32)
        square[pl.ds(0, experts), pl.ds(tok + 1 + at, 1)] = kept
        mass = mass - kept
    notes[0, 0] = square[...].astype(jnp.bfloat16)
    for way in range(2):
        note_copy(way, 1).start()
    for way in range(2):
        gather_copy(way, 1, 1, side_of(way, 0)).start()
    peer_note(0).start()
    for c in range(2):
        peer_copy(0, 1, c).start()

    def arrive(hop, j, part):
        for way in range(2):
            k, c = sign[way] * hop, side_of(way, part)
            gather_copy(way, hop, j, c).wait_recv()
            if hop + 1 < hops or (hop + 1 == hops and part == 0):
                gather_copy(way, hop + 1, j, c).start()
            peer_copy(k, j, c).start()
            if j == 0 and ((part == 1 and hop < hops) or (hop == hops and way == 0)):
                note_copy(way, hop).wait_recv()
                if hop + 1 < hops or (hop + 1 == hops and way == 0):
                    note_copy(way, hop + 1).start()
                peer_note(k).start()

    arrive(1, 0, 0)
    arrive(1, 0, 1)
    for way in range(2):
        gather_copy(way, 1, 1, side_of(way, 1)).start()

    for i in range(plan.pairs):
        n = plan.routed_tiles + i
        units = pl.ds(pl.multiple_of((2 * i + sub) * LANES, LANES), LANES)
        for side in range(2):
            if i == 0:
                small[4 + side].wait()
            wt[n, :, pl.ds(side * LANES, LANES)] = jnp.transpose(stage[side, units, :])
    for i, (at, wide) in enumerate(plan.rest):
        n = plan.routed_tiles + plan.pairs + i
        if wide < LANES:
            wt[n] = jnp.zeros_like(wt[n])
            wd[pl.ds(n * LANES + wide, LANES - wide), :] = jnp.zeros(
                (LANES - wide, width), jnp.bfloat16
            )
        for side in range(2):
            if i == 0 and plan.pairs == 0:
                small[4 + side].wait()
            wt[n, :, pl.ds(side * LANES, wide)] = jnp.transpose(stage[side, pl.ds(at, wide), :])

    events = {}

    def at_slot(spot, event):
        events.setdefault(spot, []).append(event)

    def ready(step):
        for i in range(plan.group):
            k, j = plan.order[step * plan.group + i]
            for c in range(2):
                peer_copy(k, j, c).wait_recv()
            if j == 0:
                peer_note(k).wait_recv()
            for r in range(2):
                tile = notes[r, k].astype(jnp.float32)
                mine = lax.broadcasted_iota(jnp.int32, tile.shape, 0) == me
                line = jnp.sum(jnp.where(mine, tile, 0.0), axis=0, keepdims=True)
                row = lax.broadcasted_iota(jnp.int32, (half, LANES), 0) + j * half
                lane = lax.broadcasted_iota(jnp.int32, (half, LANES), 1)
                column = jnp.sum(jnp.where(row == lane, line, 0.0), axis=1, keepdims=True)
                scale[pl.ds((2 * i + r) * half, half), :] = jnp.broadcast_to(column, (half, LANES))

    arrivals = []
    for hop in range(2, hops + 1):
        arrivals.append((hop, 0, 0))
        if hop > 2:
            arrivals.append((hop - 2, 1, 1))
        if hop < hops:
            arrivals.append((hop, 0, 1))
        arrivals.append((hop - 1, 1, 0))
    arrivals += [(hops - 1, 1, 1), (hops, 1, 0)]
    spots = []
    for i, (hop, j, part) in enumerate(arrivals):
        due = SLOTS * min(plan.step_of(hop, j), plan.step_of(-hop, j))
        spots.append(min(due, GATHER[i] if i < len(GATHER) else i))
    for i in reversed(range(len(spots) - 1)):
        spots[i] = min(spots[i], spots[i + 1])
    for (hop, j, part), spot in zip(arrivals, spots):
        at_slot(spot, functools.partial(arrive, hop, j, part))
    for step in range(plan.steps):
        at_slot(SLOTS * step, functools.partial(ready, step))
    quarter = 4

    def loads(first, last):
        for n in range(first, min(last, tiles)):
            for copy in tile_loads(n):
                copy.wait()

    for part in range(3):
        last = tiles if part == 2 else quarter * (part + 1)
        at_slot(part, functools.partial(loads, quarter * part, last))
    for copy in down_loads:
        at_slot(2, copy.wait)

    def own_part(k, j, c):
        q = plan.index(k, j)
        part_copy(q, c).wait_recv()
        value = y_all[plan.span(0, k, j), plan.cols(c)].astype(jnp.float32)
        return value + from_peer[pl.ds(q * half, half), plan.cols(c)].astype(jnp.float32)

    def pass_on(hop, j, c):
        for way in ways_of(hop, c):
            value = own_part(-sign[way] * hop, j, c)
            if hop < hops and way in ways_of(hop + 1, c):
                sum_copy(way, hop + 1, j, c).wait_recv()
                spot = (way, hop, pl.ds(j * half, half), plan.cols(c))
                value = value + coming[spot].astype(jnp.float32)
            spot = (way, hop - 1, pl.ds(j * half, half), plan.cols(c))
            going[spot] = value.astype(going.dtype)
            sum_copy(way, hop, j, c).start()

    def finish(j, c):
        value = own_part(0, j, c)
        for way in ways_of(1, c):
            sum_copy(way, 1, j, c).wait_recv()
            spot = (way, 0, pl.ds(j * half, half), plan.cols(c))
            value = value + coming[spot].astype(jnp.float32)
        out_ref[pl.ds(j * half, half), plan.cols(c)] = value.astype(out_ref.dtype)

    def chain(j):
        made = [
            functools.partial(pass_on, h, j, c) for h in range(hops, 0, -1) for c in range(2)
        ]
        return made + [functools.partial(finish, j, c) for c in range(2)]

    first, second = chain(0), chain(1)
    base = SLOTS * (plan.step_of(hops, 0) + 1)
    for at in SCATTER:
        if base + at < SLOTS * plan.steps and first:
            at_slot(base + at, first.pop(0))

    def run(t, slot):
        for step in range(plan.steps):
            todo = events.get(SLOTS * step + slot, [])
            if todo:

                @pl.when(t == step)
                def _():
                    for event in todo:
                        event()

    own_row = (lax.broadcasted_iota(jnp.int32, (plan.rows, LANES), 0) // half) % 2 == 0
    lane = lax.broadcasted_iota(jnp.int32, (plan.rows, LANES), 1)

    def activate(n):
        both = rbuf[...]
        value = silu(both[:, :LANES]) * both[:, LANES:]
        if n < plan.routed_tiles:
            value = value * scale[...]
        elif n >= plan.routed_tiles + plan.pairs:
            wide = plan.rest[n - plan.routed_tiles - plan.pairs][1]
            value = jnp.where(own_row & (lane < wide), value, 0.0)
        act[:, pl.ds(n * LANES, LANES)] = value.astype(jnp.bfloat16)

    def step_body(t, carry):
        rows = pl.ds(pl.multiple_of(t * plan.rows, plan.rows), plan.rows)
        run(t, 0)
        for n in range(tiles):

            @pl.when(t >= 0)
            def _():
                if n > 0:
                    activate(n - 1)
                rbuf[...] = jnp.dot(x_all[rows, :], wt[n], preferred_element_type=jnp.float32)

            if (n + 1) % quarter == 0 and (n + 1) // quarter < SLOTS - 1:
                run(t, (n + 1) // quarter)
        activate(tiles - 1)
        for n in range(plan.downs):
            cols = pl.ds(n * 256, 256)

            @pl.when(t >= 0)
            def _():
                y_all[rows, cols] = jnp.dot(
                    act[...], wd[:, cols], preferred_element_type=jnp.float32
                ).astype(jnp.bfloat16)

            if 2 * (n + 1) == plan.downs:
                for i in range(plan.group):
                    part_copy(plan.group * t + i, 0).start()
                run(t, SLOTS - 1)
        for i in range(plan.group):
            part_copy(plan.group * t + i, 1).start()
        return carry

    lax.fori_loop(0, plan.steps, step_body, 0)

    while first or second:
        if len(second) >= len(first):
            for event in second[:2]:
                event()
            second = second[2:]
        else:
            first.pop(0)()

    total = jnp.zeros((plan.sublanes, LANES), jnp.float32)
    for r in range(2):
        for k in range(chips):
            total = total + notes[r, k].astype(jnp.float32)
    mass = total[:, tok + 1 : tok + 2] + total[:, tok + 2 : tok + 3] + total[:, tok + 3 : tok + 4]
    every = float(tok * chips * 2)
    penalty = experts * jnp.sum(total[:, tok : tok + 1] * mass) / (plan.choose * every * every)
    pen_ref[...] = jnp.full((8, LANES), penalty, jnp.float32)

    for hop in range(1, hops + 1):
        for way in range(2):
            if hop < hops or way == 0:
                note_copy(way, hop).wait_send()
            for j in range(2):
                for c in range(2):
                    if way in ways_of(hop, c):
                        gather_copy(way, hop, j, c).wait_send()
                        sum_copy(way, hop, j, c).wait_send()
    for k in range(chips):
        peer_note(k).wait_send()
        for j in range(2):
            for c in range(2):
                peer_copy(k, j, c).wait_send()
    for q in range(len(plan.order)):
        for c in range(2):
            part_copy(q, c).wait_send()


def on_device(
    fold, hidden_state, norm_gain, router_weight, expert_ids, live_counts,
    routed_gate_up, routed_down, shared_weights,
):
    tok, width = hidden_state.shape
    chips, subs = lax.axis_size("expert"), lax.axis_size("sub")
    units, shared = routed_down.shape[1], shared_weights.shape[2]
    if subs != 2 or chips % 4 or routed_gate_up.shape[0] != 1 or tok + 4 > LANES:
        raise ValueError("unsupported sizes")
    plan = Plan(
        chips, fold, tok, width, units, shared, expert_ids.shape[1], router_weight.shape[1]
    )
    hops, count = plan.hops, len(plan.order)
    bf16, f32 = jnp.bfloat16, jnp.float32
    hbm = pl.BlockSpec(memory_space=pl.ANY)
    dma = pltpu.SemaphoreType.DMA
    mixed, penalty = pl.pallas_call(
        functools.partial(layer_kernel, plan),
        out_shape=(
            pltpu.VMEM((tok, width), bf16),
            pltpu.VMEM((8, LANES), f32),
        ),
        in_specs=[hbm] * 4 + [pl.BlockSpec(memory_space=pltpu.SMEM)] + [hbm] * 3,
        out_specs=(
            pl.BlockSpec(memory_space=pltpu.VMEM),
            pl.BlockSpec(memory_space=pltpu.VMEM),
        ),
        scratch_shapes=[
            pltpu.VMEM((tok, width), bf16),
            pltpu.VMEM((1, width), f32),
            pltpu.VMEM(router_weight.shape[::-1], bf16),
            pltpu.VMEM(expert_ids.shape[::-1], jnp.int32),
            pltpu.VMEM((plan.sublanes, LANES), f32),
            pltpu.VMEM((2, chips, plan.sublanes, LANES), bf16),
            pltpu.VMEM((plan.tiles, width, 2 * LANES), bf16),
            pltpu.VMEM((plan.depth, width), bf16),
            pltpu.VMEM((2, shared, width), bf16),
            pltpu.VMEM((count * 2 * plan.half, width), bf16),
            pltpu.VMEM((count * 2 * plan.half, width), bf16),
            pltpu.VMEM((count * plan.half, width), bf16),
            pltpu.VMEM((2, hops, tok, width), bf16),
            pltpu.VMEM((2, hops, tok, width), bf16),
            pltpu.VMEM((plan.rows, plan.depth), bf16),
            pltpu.VMEM((plan.rows, 2 * LANES), f32),
            pltpu.VMEM((plan.rows, LANES), f32),
            dma((7 + plan.pairs + len(plan.rest),)),
            dma((plan.tiles, 2)),
            dma((2, hops, 5)),
            dma((2, hops, 5)),
            dma((chips, 5)),
            dma((chips, 5)),
            dma((count, 2)),
            dma((count, 2)),
            dma((2, hops, 4)),
            dma((2, hops, 4)),
        ],
        compiler_params=pltpu.CompilerParams(
            collective_id=0, has_side_effects=True, vmem_limit_bytes=127 * 512 * 1024
        ),
        name="moe_layer",
    )(
        hidden_state, norm_gain.reshape(1, width), router_weight.T, expert_ids.T, live_counts,
        routed_gate_up, routed_down, jnp.swapaxes(shared_weights, 1, 2),
    )
    return mixed, penalty[0, :1]


def fold_of(mesh):
    chips = mesh.shape["expert"]
    try:
        spots = [tuple(d.coords) for d in mesh.devices[0, :, 0].flat]
    except (AttributeError, TypeError, ValueError):
        spots = []
    if chips % 2 or chips < 4:
        return 1
    if len(spots) == chips:
        apart = sum(abs(a - b) for a, b in zip(spots[0], spots[2]))
        return 2 if apart == 1 else 1
    return 1


def solution(mesh):
    placed = (
        P(("groups", "expert", "sub"), None),
        P(),
        P(),
        P(("groups", "expert", "sub"), None),
        P(("groups", "expert", "sub")),
        P(("expert", "sub"), None, None),
        P(("expert", "sub"), None, None),
        P(None, None, "expert"),
    )
    return jax.shard_map(
        functools.partial(on_device, fold_of(mesh)),
        mesh=mesh,
        in_specs=placed,
        out_specs=(P(("groups", "expert", "sub"), None), P("groups")),
        check_vma=False,
    )
```

```python
import functools

import jax
import jax.numpy as jnp
from jax import lax
from jax.experimental import pallas as pl
from jax.experimental.pallas import tpu as pltpu
from jax.sharding import PartitionSpec as P

MESH = pl.DeviceIdType.MESH
LANES = 128
SLOTS = 5
GATHER = (1, 2, 2, 4, 4, 5, 6, 7, 8, 9, 12, 13)
SCATTER = (1, 1, 4, 4)


def ring_place(chip, chips, fold):
    if fold == 1:
        return chip
    row, step = chip % 2, chip // 2
    return (1 - row) * step + row * (chips - 1 - step)


def ring_chip(place, chips, fold):
    if fold == 1:
        return place
    back = place // (chips // 2)
    step = (1 - back) * place + back * (chips - 1 - place)
    return 2 * step + back


class Plan:
    def __init__(self, chips, fold, tok, width, units, shared, choose, experts):
        self.chips, self.fold, self.hops = chips, fold, chips // 2
        self.tok, self.width, self.half = tok, width, tok // 2
        self.units, self.shared, self.choose, self.experts = units, shared, choose, experts
        self.sublanes = -(-experts // 16) * 16
        hops = self.hops
        order = [(0, 0), (0, 1)]
        for hop, j in (
            [(1, 0), (1, 1)]
            + [(h, 0) for h in range(2, hops + 1)]
            + [(h, 1) for h in range(2, hops + 1)]
        ):
            order.append((hop, j))
            if hop < hops:
                order.append((chips - hop, j))
        self.order = order
        self.group = 4
        self.steps = len(order) // self.group
        self.rows = self.group * 2 * self.half
        self.routed_tiles = units // LANES
        full = shared // LANES
        self.pairs = full // 2
        self.rest = [
            (at, min(LANES, shared - at)) for at in range(self.pairs * 2 * LANES, shared, LANES)
        ]
        self.tiles = self.routed_tiles + self.pairs + len(self.rest)
        self.depth = self.tiles * LANES
        self.downs = width // 256

    def index(self, k, j):
        return self.order.index((k % self.chips, j))

    def span(self, r, k, j):
        return pl.ds((2 * self.index(k, j) + r) * self.half, self.half)

    def cols(self, c):
        return pl.ds(c * (self.width // 2), self.width // 2)

    def step_of(self, k, j):
        return self.index(k, j) // self.group


def silu(v):
    return v / (1.0 + jnp.exp(-v))


def layer_kernel(
    plan, hid_hbm, gain_hbm, router_hbm, ids_hbm, live_ref, gu_hbm, dn_hbm, sh_hbm,
    out_ref, pen_ref,
    hid, gain, router, ids, square, notes, wt, wd, stage, x_all, y_all, from_peer, going, coming,
    act, rbuf, scale, in_sem, w_sem, gs, gr, ps, pr, ys, yr, ss, sr,
):
    chips, fold, hops, half = plan.chips, plan.fold, plan.hops, plan.half
    tok, width, tiles = plan.tok, plan.width, plan.tiles
    sub = lax.axis_index("sub")
    chip = lax.axis_index("expert")
    me = chip * 2 + sub
    place = ring_place(chip, chips, fold)
    right = ring_chip((place + 1) % chips, chips, fold)
    left = ring_chip((place + chips - 1) % chips, chips, fold)
    along = [{"expert": right, "sub": sub}, {"expert": left, "sub": sub}]
    peer = {"expert": chip, "sub": 1 - sub}
    sign = (-1, 1)

    def remote(src, dst, send, recv, device):
        return pltpu.make_async_remote_copy(
            src_ref=src, dst_ref=dst, send_sem=send, recv_sem=recv,
            device_id=device, device_id_type=MESH,
        )

    def gather_copy(way, hop, j, c):
        cols, at = plan.cols(c), 2 * j + c
        src = x_all.at[plan.span(0, sign[way] * (hop - 1), j), cols]
        dst = x_all.at[plan.span(0, sign[way] * hop, j), cols]
        return remote(src, dst, gs.at[way, hop - 1, at], gr.at[way, hop - 1, at], along[way])

    def note_copy(way, hop):
        src = notes.at[0, sign[way] * (hop - 1) % chips]
        dst = notes.at[0, sign[way] * hop % chips]
        return remote(src, dst, gs.at[way, hop - 1, 4], gr.at[way, hop - 1, 4], along[way])

    def peer_copy(k, j, c):
        k, cols, at = k % chips, plan.cols(c), 2 * j + c
        return remote(
            x_all.at[plan.span(0, k, j), cols], x_all.at[plan.span(1, k, j), cols],
            ps.at[k, at], pr.at[k, at], peer,
        )

    def peer_note(k):
        k = k % chips
        return remote(notes.at[0, k], notes.at[1, k], ps.at[k, 4], pr.at[k, 4], peer)

    def part_copy(q, c):
        cols = plan.cols(c)
        if isinstance(q, int):
            src, dst = pl.ds((2 * q + 1) * half, half), pl.ds(q * half, half)
        else:
            src = pl.ds(pl.multiple_of((2 * q + 1) * half, half), half)
            dst = pl.ds(pl.multiple_of(q * half, half), half)
        return remote(
            y_all.at[src, cols], from_peer.at[dst, cols], ys.at[q, c], yr.at[q, c], peer
        )

    def sum_copy(way, hop, j, c):
        spot = (way, hop - 1, pl.ds(j * half, half), plan.cols(c))
        at = 2 * j + c
        return remote(
            going.at[spot], coming.at[spot], ss.at[way, hop - 1, at], sr.at[way, hop - 1, at],
            along[way],
        )

    def side_of(way, part):
        return way if part == 0 else 1 - way

    def ways_of(hop, c):
        return (c,) if hop == hops else (0, 1)

    small = [
        pltpu.make_async_copy(hid_hbm, hid, in_sem.at[0]),
        pltpu.make_async_copy(gain_hbm, gain, in_sem.at[1]),
        pltpu.make_async_copy(router_hbm, router, in_sem.at[2]),
        pltpu.make_async_copy(ids_hbm, ids, in_sem.at[3]),
        pltpu.make_async_copy(sh_hbm.at[0], stage.at[0], in_sem.at[4]),
        pltpu.make_async_copy(sh_hbm.at[1], stage.at[1], in_sem.at[5]),
    ]
    down_loads = [pltpu.make_async_copy(dn_hbm.at[0], wd.at[pl.ds(0, plan.units)], in_sem.at[6])]
    for i in range(plan.pairs):
        down_loads.append(
            pltpu.make_async_copy(
                sh_hbm.at[2, pl.ds(pl.multiple_of((2 * i + sub) * LANES, LANES), LANES)],
                wd.at[pl.ds(plan.units + i * LANES, LANES)], in_sem.at[7 + i],
            )
        )
    for i, (at, wide) in enumerate(plan.rest):
        n = plan.routed_tiles + plan.pairs + i
        down_loads.append(
            pltpu.make_async_copy(
                sh_hbm.at[2, pl.ds(at, wide)], wd.at[pl.ds(n * LANES, wide)],
                in_sem.at[7 + plan.pairs + i],
            )
        )

    def tile_loads(n):
        if n < plan.routed_tiles:
            return [
                pltpu.make_async_copy(
                    gu_hbm.at[0, :, pl.ds(side * plan.units + n * LANES, LANES)],
                    wt.at[n, :, pl.ds(side * LANES, LANES)], w_sem.at[n, side],
                )
                for side in range(2)
            ]
        return []

    for copy in small[:4]:
        copy.start()
    barrier = pltpu.get_barrier_semaphore()
    for target in along + [peer]:
        pl.semaphore_signal(barrier, inc=1, device_id=target, device_id_type=MESH)
    small[4].start()
    small[5].start()
    for n in range(tiles):
        for copy in tile_loads(n):
            copy.start()
    for copy in down_loads:
        copy.start()

    small[0].wait()
    small[1].wait()
    for j in range(2):
        values = hid[pl.ds(j * half, half), :].astype(jnp.float32)
        spread = jnp.mean(values * values, axis=-1, keepdims=True)
        x_all[plan.span(0, 0, j), :] = (
            values * lax.rsqrt(spread + 1e-06) * gain[...]
        ).astype(jnp.bfloat16)
    pl.semaphore_wait(barrier, 3)
    for part in range(2):
        for way in range(2):
            gather_copy(way, 1, 0, side_of(way, part)).start()
    for c in range(2):
        peer_copy(0, 0, c).start()

    small[2].wait()
    small[3].wait()
    experts = plan.experts
    expert = lax.broadcasted_iota(jnp.int32, (experts, half), 0)
    square[...] = jnp.zeros_like(square)
    load = jnp.zeros((experts, 1), jnp.float32)
    mass = jnp.zeros((experts, 1), jnp.float32)
    named = ids[...]
    for j in range(2):
        logits = lax.dot_general(
            router[...], x_all[plan.span(0, 0, j), :], (((1,), (1,)), ((), ())),
            preferred_element_type=jnp.float32,
        )
        probs = 1.0 / (1.0 + jnp.exp(-logits))
        hot = jnp.zeros((experts, half), jnp.float32)
        for k in range(plan.choose):
            hot = hot + jnp.where(named[k : k + 1, j * half : (j + 1) * half] == expert, 1.0, 0.0)
        token = lax.broadcasted_iota(jnp.int32, (experts, half), 1) + j * half
        live = jnp.where(token < live_ref[0], 1.0, 0.0)
        picked = hot * probs
        weights = live * picked / jnp.sum(picked, axis=0, keepdims=True)
        square[pl.ds(0, experts), pl.ds(j * half, half)] = weights
        load = load + jnp.sum(hot * live, axis=1, keepdims=True)
        mass = mass + jnp.sum(probs * live, axis=1, keepdims=True)
    square[pl.ds(0, experts), pl.ds(tok, 1)] = load
    for at in range(3):
        kept = mass.astype(jnp.bfloat16).astype(jnp.float32)
        square[pl.ds(0, experts), pl.ds(tok + 1 + at, 1)] = kept
        mass = mass - kept
    notes[0, 0] = square[...].astype(jnp.bfloat16)
    for way in range(2):
        note_copy(way, 1).start()
    for way in range(2):
        gather_copy(way, 1, 1, side_of(way, 0)).start()
    peer_note(0).start()
    for c in range(2):
        peer_copy(0, 1, c).start()

    def arrive(hop, j, part):
        for way in range(2):
            k, c = sign[way] * hop, side_of(way, part)
            gather_copy(way, hop, j, c).wait_recv()
            if hop + 1 < hops or (hop + 1 == hops and part == 0):
                gather_copy(way, hop + 1, j, c).start()
            peer_copy(k, j, c).start()
            if j == 0 and ((part == 1 and hop < hops) or (hop == hops and way == 0)):
                note_copy(way, hop).wait_recv()
                if hop + 1 < hops or (hop + 1 == hops and way == 0):
                    note_copy(way, hop + 1).start()
                peer_note(k).start()

    arrive(1, 0, 0)
    arrive(1, 0, 1)
    for way in range(2):
        gather_copy(way, 1, 1, side_of(way, 1)).start()

    for i in range(plan.pairs):
        n = plan.routed_tiles + i
        units = pl.ds(pl.multiple_of((2 * i + sub) * LANES, LANES), LANES)
        for side in range(2):
            if i == 0:
                small[4 + side].wait()
            wt[n, :, pl.ds(side * LANES, LANES)] = jnp.transpose(stage[side, units, :])
    for i, (at, wide) in enumerate(plan.rest):
        n = plan.routed_tiles + plan.pairs + i
        if wide < LANES:
            wt[n] = jnp.zeros_like(wt[n])
            wd[pl.ds(n * LANES + wide, LANES - wide), :] = jnp.zeros(
                (LANES - wide, width), jnp.bfloat16
            )
        for side in range(2):
            if i == 0 and plan.pairs == 0:
                small[4 + side].wait()
            wt[n, :, pl.ds(side * LANES, wide)] = jnp.transpose(stage[side, pl.ds(at, wide), :])

    events = {}

    def at_slot(spot, event):
        events.setdefault(spot, []).append(event)

    def ready(step):
        for i in range(plan.group):
            k, j = plan.order[step * plan.group + i]
            for c in range(2):
                peer_copy(k, j, c).wait_recv()
            if j == 0:
                peer_note(k).wait_recv()
            for r in range(2):
                tile = notes[r, k].astype(jnp.float32)
                mine = lax.broadcasted_iota(jnp.int32, tile.shape, 0) == me
                line = jnp.sum(jnp.where(mine, tile, 0.0), axis=0, keepdims=True)
                row = lax.broadcasted_iota(jnp.int32, (half, LANES), 0) + j * half
                lane = lax.broadcasted_iota(jnp.int32, (half, LANES), 1)
                column = jnp.sum(jnp.where(row == lane, line, 0.0), axis=1, keepdims=True)
                scale[pl.ds((2 * i + r) * half, half), :] = jnp.broadcast_to(column, (half, LANES))

    arrivals = []
    for hop in range(2, hops + 1):
        arrivals.append((hop, 0, 0))
        if hop > 2:
            arrivals.append((hop - 2, 1, 1))
        if hop < hops:
            arrivals.append((hop, 0, 1))
        arrivals.append((hop - 1, 1, 0))
    arrivals += [(hops - 1, 1, 1), (hops, 1, 0)]
    spots = []
    for i, (hop, j, part) in enumerate(arrivals):
        due = SLOTS * min(plan.step_of(hop, j), plan.step_of(-hop, j))
        spots.append(min(due, GATHER[i] if i < len(GATHER) else i))
    for i in reversed(range(len(spots) - 1)):
        spots[i] = min(spots[i], spots[i + 1])
    for (hop, j, part), spot in zip(arrivals, spots):
        at_slot(spot, functools.partial(arrive, hop, j, part))
    for step in range(plan.steps):
        at_slot(SLOTS * step, functools.partial(ready, step))
    quarter = 4

    def loads(first, last):
        for n in range(first, min(last, tiles)):
            for copy in tile_loads(n):
                copy.wait()

    for part in range(3):
        last = tiles if part == 2 else quarter * (part + 1)
        at_slot(part, functools.partial(loads, quarter * part, last))
    for copy in down_loads:
        at_slot(2, copy.wait)

    def own_part(k, j, c):
        q = plan.index(k, j)
        part_copy(q, c).wait_recv()
        value = y_all[plan.span(0, k, j), plan.cols(c)].astype(jnp.float32)
        return value + from_peer[pl.ds(q * half, half), plan.cols(c)].astype(jnp.float32)

    def pass_on(hop, j, c):
        for way in ways_of(hop, c):
            value = own_part(-sign[way] * hop, j, c)
            if hop < hops and way in ways_of(hop + 1, c):
                sum_copy(way, hop + 1, j, c).wait_recv()
                spot = (way, hop, pl.ds(j * half, half), plan.cols(c))
                value = value + coming[spot].astype(jnp.float32)
            spot = (way, hop - 1, pl.ds(j * half, half), plan.cols(c))
            going[spot] = value.astype(going.dtype)
            sum_copy(way, hop, j, c).start()

    def finish(j, c):
        value = own_part(0, j, c)
        for way in ways_of(1, c):
            sum_copy(way, 1, j, c).wait_recv()
            spot = (way, 0, pl.ds(j * half, half), plan.cols(c))
            value = value + coming[spot].astype(jnp.float32)
        out_ref[pl.ds(j * half, half), plan.cols(c)] = value.astype(out_ref.dtype)

    def chain(j):
        made = [
            functools.partial(pass_on, h, j, c) for h in range(hops, 0, -1) for c in range(2)
        ]
        return made + [functools.partial(finish, j, c) for c in range(2)]

    first, second = chain(0), chain(1)
    base = SLOTS * (plan.step_of(hops, 0) + 1)
    for at in SCATTER:
        if base + at < SLOTS * plan.steps and first:
            at_slot(base + at, first.pop(0))

    def run(t, slot):
        for step in range(plan.steps):
            todo = events.get(SLOTS * step + slot, [])
            if todo:

                @pl.when(t == step)
                def _():
                    for event in todo:
                        event()

    own_row = (lax.broadcasted_iota(jnp.int32, (plan.rows, LANES), 0) // half) % 2 == 0
    lane = lax.broadcasted_iota(jnp.int32, (plan.rows, LANES), 1)

    def activate(n):
        both = rbuf[...]
        value = silu(both[:, :LANES]) * both[:, LANES:]
        if n < plan.routed_tiles:
            value = value * scale[...]
        elif n >= plan.routed_tiles + plan.pairs:
            wide = plan.rest[n - plan.routed_tiles - plan.pairs][1]
            value = jnp.where(own_row & (lane < wide), value, 0.0)
        act[:, pl.ds(n * LANES, LANES)] = value.astype(jnp.bfloat16)

    def step_body(t, carry):
        rows = pl.ds(pl.multiple_of(t * plan.rows, plan.rows), plan.rows)
        run(t, 0)
        for n in range(tiles):

            @pl.when(t >= 0)
            def _():
                if n > 0:
                    activate(n - 1)
                rbuf[...] = jnp.dot(x_all[rows, :], wt[n], preferred_element_type=jnp.float32)

            if (n + 1) % quarter == 0 and (n + 1) // quarter < SLOTS - 1:
                run(t, (n + 1) // quarter)
        activate(tiles - 1)
        for n in range(plan.downs):
            cols = pl.ds(n * 256, 256)

            @pl.when(t >= 0)
            def _():
                y_all[rows, cols] = jnp.dot(
                    act[...], wd[:, cols], preferred_element_type=jnp.float32
                ).astype(jnp.bfloat16)

            if 2 * (n + 1) == plan.downs:
                for i in range(plan.group):
                    part_copy(plan.group * t + i, 0).start()
                run(t, SLOTS - 1)
        for i in range(plan.group):
            part_copy(plan.group * t + i, 1).start()
        return carry

    lax.fori_loop(0, plan.steps, step_body, 0)

    def totals():
        total = jnp.zeros((plan.sublanes, LANES), jnp.float32)
        for r in range(2):
            for k in range(chips):
                total = total + notes[r, k].astype(jnp.float32)
        mass = total[:, tok + 1 : tok + 2] + total[:, tok + 2 : tok + 3] + total[:, tok + 3 : tok + 4]
        every = float(tok * chips * 2)
        penalty = experts * jnp.sum(total[:, tok : tok + 1] * mass) / (plan.choose * every * every)
        pen_ref[...] = jnp.full((8, LANES), penalty, jnp.float32)

    rounds = 0
    while first or second:
        if len(first) % 2:
            first.pop(0)()
        for event in second[:2] + first[:2]:
            event()
        second, first = second[2:], first[2:]
        rounds += 1
        if rounds == 2:
            totals()

    for hop in range(1, hops + 1):
        for way in range(2):
            if hop < hops or way == 0:
                note_copy(way, hop).wait_send()
            for j in range(2):
                for c in range(2):
                    if way in ways_of(hop, c):
                        gather_copy(way, hop, j, c).wait_send()
                        sum_copy(way, hop, j, c).wait_send()
    for k in range(chips):
        peer_note(k).wait_send()
        for j in range(2):
            for c in range(2):
                peer_copy(k, j, c).wait_send()
    for q in range(len(plan.order)):
        for c in range(2):
            part_copy(q, c).wait_send()


def on_device(
    fold, hidden_state, norm_gain, router_weight, expert_ids, live_counts,
    routed_gate_up, routed_down, shared_weights,
):
    tok, width = hidden_state.shape
    chips, subs = lax.axis_size("expert"), lax.axis_size("sub")
    units, shared = routed_down.shape[1], shared_weights.shape[2]
    if subs != 2 or chips % 4 or routed_gate_up.shape[0] != 1 or tok + 4 > LANES:
        raise ValueError("unsupported sizes")
    plan = Plan(
        chips, fold, tok, width, units, shared, expert_ids.shape[1], router_weight.shape[1]
    )
    hops, count = plan.hops, len(plan.order)
    bf16, f32 = jnp.bfloat16, jnp.float32
    hbm = pl.BlockSpec(memory_space=pl.ANY)
    dma = pltpu.SemaphoreType.DMA
    mixed, penalty = pl.pallas_call(
        functools.partial(layer_kernel, plan),
        out_shape=(
            pltpu.VMEM((tok, width), bf16),
            pltpu.VMEM((8, LANES), f32),
        ),
        in_specs=[hbm] * 4 + [pl.BlockSpec(memory_space=pltpu.SMEM)] + [hbm] * 3,
        out_specs=(
            pl.BlockSpec(memory_space=pltpu.VMEM),
            pl.BlockSpec(memory_space=pltpu.VMEM),
        ),
        scratch_shapes=[
            pltpu.VMEM((tok, width), bf16),
            pltpu.VMEM((1, width), f32),
            pltpu.VMEM(router_weight.shape[::-1], bf16),
            pltpu.VMEM(expert_ids.shape[::-1], jnp.int32),
            pltpu.VMEM((plan.sublanes, LANES), f32),
            pltpu.VMEM((2, chips, plan.sublanes, LANES), bf16),
            pltpu.VMEM((plan.tiles, width, 2 * LANES), bf16),
            pltpu.VMEM((plan.depth, width), bf16),
            pltpu.VMEM((2, shared, width), bf16),
            pltpu.VMEM((count * 2 * plan.half, width), bf16),
            pltpu.VMEM((count * 2 * plan.half, width), bf16),
            pltpu.VMEM((count * plan.half, width), bf16),
            pltpu.VMEM((2, hops, tok, width), bf16),
            pltpu.VMEM((2, hops, tok, width), bf16),
            pltpu.VMEM((plan.rows, plan.depth), bf16),
            pltpu.VMEM((plan.rows, 2 * LANES), f32),
            pltpu.VMEM((plan.rows, LANES), f32),
            dma((7 + plan.pairs + len(plan.rest),)),
            dma((plan.tiles, 2)),
            dma((2, hops, 5)),
            dma((2, hops, 5)),
            dma((chips, 5)),
            dma((chips, 5)),
            dma((count, 2)),
            dma((count, 2)),
            dma((2, hops, 4)),
            dma((2, hops, 4)),
        ],
        compiler_params=pltpu.CompilerParams(
            collective_id=0, has_side_effects=True, vmem_limit_bytes=127 * 512 * 1024
        ),
        name="moe_layer",
    )(
        hidden_state, norm_gain.reshape(1, width), router_weight.T, expert_ids.T, live_counts,
        routed_gate_up, routed_down, jnp.swapaxes(shared_weights, 1, 2),
    )
    return mixed, penalty[0, :1]


def fold_of(mesh):
    chips = mesh.shape["expert"]
    try:
        spots = [tuple(d.coords) for d in mesh.devices[0, :, 0].flat]
    except (AttributeError, TypeError, ValueError):
        spots = []
    if chips % 2 or chips < 4:
        return 1
    if len(spots) == chips:
        apart = sum(abs(a - b) for a, b in zip(spots[0], spots[2]))
        return 2 if apart == 1 else 1
    return 1


def solution(mesh):
    placed = (
        P(("groups", "expert", "sub"), None),
        P(),
        P(),
        P(("groups", "expert", "sub"), None),
        P(("groups", "expert", "sub")),
        P(("expert", "sub"), None, None),
        P(("expert", "sub"), None, None),
        P(None, None, "expert"),
    )
    return jax.shard_map(
        functools.partial(on_device, fold_of(mesh)),
        mesh=mesh,
        in_specs=placed,
        out_specs=(P(("groups", "expert", "sub"), None), P("groups")),
        check_vma=False,
    )
```
